32 devices in a mesh: gx: 4 (over z), gy: 4 (over x, core), gz: 2 (over y).
Axes of the slice: x: 2, y: 2, z: 4, core: 2. Of those that a mesh axis runs over, the one named last changes fastest.
Arguments:
- weights: float32 [3, 16, 128, 512], P(None, 'gx', 'gz', 'gy'), may hold values from 0.2 to 2
- abscissas: float32 [3, 16, 128, 512], P(None, 'gx', 'gz', 'gy'), may hold values from -4 to 4, as said below
Outputs:
- moments_end: float32 [6, 16, 128, 512], P(None, 'gx', 'gz', 'gy')
The draws below stay inside these ranges and needn't reach their ends.
Inputs may be any that keep to these rules, and one draw needn't show every extreme that they name: In every cell the three abscissas increase with the node index, consecutive ones at least 0.25 apart.
All inputs are finite; a program needn't handle non-finite values. Where the reference program divides by a largest or mean magnitude, that divisor is 1e-20 or more.
Results may differ from the reference program's by a relative error of at most 0.0003.
Values sent between devices are 32-bit elements; how exact they have to be, the bound alone decides.
A program may use at most 128 MiB of HBM per device.

```python
import math
import jax
import jax.numpy as jnp
from jax import lax

NODES = 3
NX = 16
NZ = 128
NY = 512


def draw_abscissas(key, part):
    noise_key = jax.random.fold_in(key, 11)
    place_key = jax.random.fold_in(key, 23)
    height_key = jax.random.fold_in(key, 37)
    noise = jax.random.uniform(noise_key, (NODES, NX, NZ, NY), jnp.float32, -0.25, 0.25)
    centres = jnp.array([-1.0, 0.0, 1.0], jnp.float32).reshape(3, 1, 1, 1)
    position = (jnp.arange(NX, dtype=jnp.float32) + 0.5) / NX
    window_start = jax.random.randint(place_key, (), 0, NX - 3)
    height = jax.random.uniform(height_key, (), jnp.float32, 1.6, 3.2)
    cell_index = jnp.arange(NX, dtype=jnp.int32)
    inside = (cell_index >= window_start) & (cell_index < window_start + 4)
    factor = jnp.where(inside, height, 0.5 + position).reshape(1, NX, 1, 1)
    return ((centres + noise) * factor).astype(jnp.float32)


def block_scale(stream_key, dims, cuts, least, largest):
    gain = 1.0
    for dim, shards_of in cuts:
        heights = jax.random.uniform(jax.random.fold_in(jax.random.fold_in(stream_key, 6), dim), (shards_of,), jnp.float32, least / len(cuts), largest / len(cuts))
        gain = gain * jnp.repeat(jnp.exp(heights), dims[dim] // shards_of).reshape((-1,) + (1,) * (len(dims) - 1 - dim))
    return gain


def setup_inputs(seed: int = 0) -> dict:
    streams_of = jax.random.split(jax.random.key(seed), 3)
    return {
        "weights": jnp.clip(jnp.exp(math.log(2.0) - 2.3025851 * jax.random.uniform(streams_of[0], (NODES, NX, NZ, NY), jnp.float32) ** block_scale(streams_of[0], (NODES, NX, NZ, NY), ((1, 4), (2, 2), (3, 4)), -0.2, 0.2)), 0.2, 2.0),
        "abscissas": draw_abscissas(jax.random.fold_in(streams_of[2], 71), 0),
    }


COURANT = 0.4
SPEED_TOTAL = 1.72
AXIS_SPEEDS = ((1, 0.6), (2, 0.64), (3, 0.48))

def minmod(first, second):
    return jnp.where(first * second > 0.0, jnp.sign(first) * jnp.minimum(jnp.abs(first), jnp.abs(second)), 0.0)

def cut_along(array, lower, upper, array_axis):
    return lax.slice_in_dim(array, lower, upper, axis=array_axis)

def moments_of(node_weights, node_speeds):
    result = []
    power = node_weights
    for order in range(6):
        result.append(lax.optimization_barrier(jnp.sum(power, axis=0)))
        power = power * node_speeds
    return jnp.stack(result)

def face_divergence(node_weights, node_speeds):
    total = None
    for array_axis, component in AXIS_SPEEDS:
        window = [slice(None), slice(2, -2), slice(2, -2), slice(2, -2)]
        window[array_axis] = slice(None)
        line_w = node_weights[tuple(window)]
        line_u = node_speeds[tuple(window)]
        length = line_w.shape[array_axis]
        jumps = cut_along(line_w, 1, length, array_axis) - cut_along(line_w, 0, length - 1, array_axis)
        slopes = minmod(cut_along(jumps, 0, length - 2, array_axis), cut_along(jumps, 1, length - 1, array_axis))
        left_w = cut_along(line_w, 1, length - 2, array_axis) + 0.5 * cut_along(slopes, 0, length - 3, array_axis)
        right_w = cut_along(line_w, 2, length - 1, array_axis) - 0.5 * cut_along(slopes, 1, length - 2, array_axis)
        left_u = cut_along(line_u, 1, length - 2, array_axis)
        right_u = cut_along(line_u, 2, length - 1, array_axis)
        left_term = component * left_w * jnp.maximum(left_u, 0.0)
        right_term = component * right_w * jnp.minimum(right_u, 0.0)
        fluxes = []
        for order in range(6):
            fluxes.append(lax.optimization_barrier(jnp.sum(left_term + right_term, axis=0)))
            left_term = left_term * left_u
            right_term = right_term * right_u
        flux = jnp.stack(fluxes)
        faces = length - 3
        diverge = cut_along(flux, 1, faces, array_axis) - cut_along(flux, 0, faces - 1, array_axis)
        total = diverge if total is None else total + diverge
    return total

def invert(moments):
    mom = [moments[index] for index in range(6)]
    mean_one = mom[1] / mom[0]
    first_row = [None] + [mom[level + 1] - mean_one * mom[level] for level in range(1, 5)]
    mean_two = first_row[2] / first_row[1] - mean_one
    spread_one = first_row[1] / mom[0]
    second_two = first_row[3] - mean_two * first_row[2] - spread_one * mom[2]
    second_three = first_row[4] - mean_two * first_row[3] - spread_one * mom[3]
    mean_three = second_three / second_two - first_row[2] / first_row[1]
    spread_two = second_two / first_row[1]
    centre = (mean_one + mean_two + mean_three) / 3.0
    dev_one = mean_one - centre
    dev_two = mean_two - centre
    dev_three = mean_three - centre
    radius = jnp.sqrt((dev_one * dev_one + dev_two * dev_two + dev_three * dev_three + 2.0 * spread_one + 2.0 * spread_two) / 6.0)
    determinant = dev_one * dev_two * dev_three - dev_one * spread_two - dev_three * spread_one
    ratio = determinant / (2.0 * radius * radius * radius)
    angle = jnp.arccos(ratio) / 3.0
    highest = centre + 2.0 * radius * jnp.cos(angle)
    lowest = centre + 2.0 * radius * jnp.cos(angle + 2.0 * math.pi / 3.0)
    middle = 3.0 * centre - highest - lowest
    root_one = jnp.sqrt(spread_one)
    root_two = jnp.sqrt(spread_two)
    speeds = []
    masses = []
    for value in (lowest, middle, highest):
        first_comp = (value - mean_one) / root_one
        second_comp = ((value - mean_two) * first_comp - root_one) / root_two
        masses.append(mom[0] / (1.0 + first_comp * first_comp + second_comp * second_comp))
        speeds.append(value)
    return (jnp.stack(masses), jnp.stack(speeds))

def periodic(array):
    return jnp.pad(array, ((0, 0), (2, 2), (2, 2), (2, 2)), mode='wrap')

def reference(weights, abscissas):
    moments_start = moments_of(weights, abscissas)
    step_one = COURANT / (SPEED_TOTAL * jnp.max(jnp.abs(abscissas)))
    moments_mid = moments_start - step_one * face_divergence(periodic(weights), periodic(abscissas))
    mid_weights, mid_speeds = invert(moments_mid)
    step_two = COURANT / (SPEED_TOTAL * jnp.max(jnp.abs(mid_speeds)))
    change = face_divergence(periodic(mid_weights), periodic(mid_speeds))
    return 0.5 * moments_start + 0.5 * (moments_mid - step_two * change)
```

```python
import functools

import jax
import jax.numpy as jnp
from jax import lax
from jax.experimental import pallas as pl
from jax.experimental.pallas import tpu as pltpu
from jax.sharding import PartitionSpec as P

MESH = pl.DeviceIdType.MESH
COURANT = 0.4
SPEED_TOTAL = 1.72
CX, CZ, CY = 0.6, 0.64, 0.48
COS_COEFFS = (
    0.500000001, 0.57735016, -0.111107418, 0.0534091939, -0.032581471,
    0.0214679648, -0.0133677689, 0.00671727328, -0.00224476683, 0.000356832615,
)
ROWS = 8


def minmod(a, b):
    return jnp.maximum(jnp.minimum(a, b), 0.0) + jnp.minimum(jnp.maximum(a, b), 0.0)


def third_cos(t):
    acc = jnp.full_like(t, COS_COEFFS[-1])
    for c in COS_COEFFS[-2::-1]:
        acc = acc * t + c
    return acc


def total(parts):
    return parts[0] + parts[1] + parts[2]


def shift(value, amount, axis):
    return pltpu.roll(value, amount % value.shape[axis], axis)


def edge_terms(own, left, right, axis, c):
    shape = own(0).shape
    q = lax.broadcasted_iota(jnp.int32, shape, axis) & 3
    q0, q1, q2 = q == 0, q == 1, q == 2
    dl, dh, dy, us, uxs = [], [], [], [], []
    for i in range(3):
        po, plw, prw = own(i), left(i), right(i)
        u, ux = own(3 + i), jnp.where(q1, left(3 + i), right(3 + i))
        bw, aw = shift(po, 1, axis), shift(po, -1, axis)
        bl, ar = shift(plw, 1, axis), shift(prw, -1, axis)
        bc, ac = jnp.where(q2, bl, bw), jnp.where(q1, ar, aw)
        sc, sw = 0.5 * minmod(po - bc, ac - po), 0.5 * minmod(po - bw, aw - po)
        px = jnp.where(q1, plw, prw)
        bx, ax = jnp.where(q1, bl, bw), jnp.where(q1, aw, ar)
        sx = 0.5 * minmod(px - bx, ax - px)
        up, um = c * jnp.maximum(u, 0.0), c * jnp.minimum(u, 0.0)
        dl.append((sc - sw) * up)
        dh.append((sw - sc) * um)
        wrong = jnp.where(q1, (po + sw) * up, (po - sw) * um)
        outer = jnp.where(
            q1, (px + sx) * (c * jnp.maximum(ux, 0.0)), (px - sx) * (c * jnp.minimum(ux, 0.0))
        )
        dy.append((outer, wrong))
        us.append(u)
        uxs.append(ux)
    result = []
    outer, wrong = [d[0] for d in dy], [d[1] for d in dy]
    for k in range(6):
        a, b = total(dl), total(dh)
        y = total(outer) - total(wrong)
        mid = a - b
        result.append(
            jnp.where(
                q0,
                shift(b, -1, axis),
                jnp.where(
                    q1,
                    mid + shift(y, -1, axis),
                    jnp.where(q2, mid - shift(y, 1, axis), -shift(a, 1, axis)),
                ),
            )
        )
        if k < 5:
            dl = [v * u for v, u in zip(dl, us)]
            dh = [v * u for v, u in zip(dh, us)]
            wrong = [v * u for v, u in zip(wrong, us)]
            outer = [v * u for v, u in zip(outer, uxs)]
    return result


def invert(m):
    inv0 = 1.0 / m[0]
    a0 = m[1] * inv0
    s = [None] + [m[l + 1] - a0 * m[l] for l in range(1, 5)]
    inv1 = 1.0 / s[1]
    lead = s[2] * inv1
    a1 = lead - a0
    b1 = s[1] * inv0
    t2 = s[3] - a1 * s[2] - b1 * m[2]
    t3 = s[4] - a1 * s[3] - b1 * m[3]
    inv2 = 1.0 / t2
    a2 = t3 * inv2 - lead
    b2 = t2 * inv1
    centre = (a0 + a1 + a2) * (1.0 / 3.0)
    d0, d1, d2 = a0 - centre, a1 - centre, a2 - centre
    square = (d0 * d0 + d1 * d1 + d2 * d2 + 2.0 * b1 + 2.0 * b2) * (1.0 / 6.0)
    radius = jnp.sqrt(square)
    det = d0 * d1 * d2 - d0 * b2 - d2 * b1
    half = det / (4.0 * square * radius)
    high = centre + 2.0 * radius * third_cos(jnp.sqrt(jnp.maximum(0.5 + half, 0.0)))
    low = centre - 2.0 * radius * third_cos(jnp.sqrt(jnp.maximum(0.5 - half, 0.0)))
    middle = 3.0 * centre - high - low
    ib1, ib2 = m[0] * inv1, s[1] * inv2
    masses = []
    for value in (low, middle, high):
        d = value - a0
        e = (value - a1) * d - b1
        masses.append(m[0] / (1.0 + ib1 * (d * d + ib2 * (e * e))))
    return masses, (low, middle, high)


def kernel(
    sizes, w_hbm, u_hbm, out_hbm, w1, u1, w2, u2, start, mid, acc, outv, ey, ez,
    packy, packz, rx, ry, rz, mx, ra, rb,
    s_in, s_out, sx_s, sx_r, sy_s, sy_r, sz_s, sz_r, sa_s, sa_r, sb_s, sb_r,
):
    ngx, ngy, ngz = sizes
    gx, gy, gz = (lax.axis_index(a) for a in ("gx", "gy", "gz"))
    _, nx, nz, ny = w1.shape
    chunks = nz // ROWS
    xdown, xup = {"gx": lax.rem(gx + ngx - 1, ngx)}, {"gx": lax.rem(gx + 1, ngx)}
    ydown, yup = {"gy": lax.rem(gy + ngy - 1, ngy)}, {"gy": lax.rem(gy + 1, ngy)}
    zdown, zup = {"gz": lax.rem(gz + ngz - 1, ngz)}, {"gz": lax.rem(gz + 1, ngz)}
    peers_a = [{"gx": lax.rem(gx + d, ngx)} for d in range(1, ngx)]
    flat = gy * ngz + gz
    peers_b = []
    for d in range(1, ngy * ngz):
        other = lax.rem(flat + d, ngy * ngz)
        peers_b.append({"gy": lax.div(other, ngz), "gz": lax.rem(other, ngz)})

    loads = [
        pltpu.make_async_copy(w_hbm, w1, s_in.at[0]),
        pltpu.make_async_copy(u_hbm, u1, s_in.at[1]),
    ]
    for copy in loads:
        copy.start()
    barrier = pltpu.get_barrier_semaphore()
    for peer in peers_a + peers_b:
        pl.semaphore_signal(barrier, inc=1, device_id=peer, device_id_type=MESH)
    loads[1].wait()

    def remote(src, dst, send, recv, peer):
        pltpu.make_async_remote_copy(
            src_ref=src, dst_ref=dst, send_sem=send, recv_sem=recv,
            device_id=peer, device_id_type=MESH,
        ).start()

    def wait_bytes(ref, sem):
        pltpu.make_async_copy(ref, ref, sem).wait()

    def send_all(src, peers, dst, send, recv):
        for d, peer in enumerate(peers):
            remote(src, dst.at[d], send, recv, peer)

    def send_x(s, c, w, u):
        rows = pl.ds(pl.multiple_of(c * ROWS, ROWS), ROWS)
        dst, send, recv = rx.at[s, c], sx_s.at[s, c], sx_r.at[s, c]
        remote(w.at[:, 0:2, rows], dst.at[:, 3:5], send, recv, xdown)
        remote(w.at[:, nx - 2 : nx, rows], dst.at[:, 0:2], send, recv, xup)
        remote(u.at[:, 0:1, rows], dst.at[:, 5:6], send, recv, xdown)
        remote(u.at[:, nx - 1 : nx, rows], dst.at[:, 2:3], send, recv, xup)

    def exchange_yz(s, w, u):
        lane = lax.broadcasted_iota(jnp.int32, (ROWS, ny), 1) >> 2

        def pack(c, held):
            rows = pl.ds(pl.multiple_of(c * ROWS, ROWS), ROWS)
            held = list(held)
            for x in range(nx):
                p = c * nx + x
                for i in range(3):
                    for j, ref in ((i, w), (3 + i, u)):
                        moved = pltpu.roll(ref[i, x, rows, :], 4 * p + 2, 1)
                        held[j] = jnp.where(lane == p, moved, held[j])
            return tuple(held)

        held = lax.fori_loop(
            0, chunks, pack, tuple(jnp.zeros((ROWS, ny), jnp.float32) for _ in range(6))
        )
        for j in range(6):
            packy[s, j] = held[j]
        for i in range(3):
            for x in range(nx):
                for j, ref in ((i, w), (3 + i, u)):
                    packz[s, j, 4 * x : 4 * x + 2, :] = ref[i, x, nz - 2 : nz, :]
                    packz[s, j, 4 * x + 2 : 4 * x + 4, :] = ref[i, x, 0:2, :]
        remote(packy.at[s], ry.at[s, 1], sy_s.at[s], sy_r.at[s], ydown)
        remote(packy.at[s], ry.at[s, 0], sy_s.at[s], sy_r.at[s], yup)
        remote(packz.at[s], rz.at[s, 1], sz_s.at[s], sz_r.at[s], zdown)
        remote(packz.at[s], rz.at[s, 0], sz_s.at[s], sz_r.at[s], zup)

    def line_terms(w, u, x, rows, axis, c):
        ls, rs, us = [], [], []
        for i in range(3):
            wv, uv = w[i, x, rows, :], u[i, x, rows, :]
            jump = wv - shift(wv, 1, axis)
            s = 0.5 * minmod(jump, shift(jump, -1, axis))
            ls.append((wv + s) * (c * jnp.maximum(uv, 0.0)))
            rs.append((wv - s) * (c * jnp.minimum(uv, 0.0)))
            us.append(uv)
        for k in range(6):
            g, h = total(ls), total(rs)
            yield k, (g - h) - shift(g, 1, axis) + shift(h, -1, axis)
            if k < 5:
                ls = [v * u_ for v, u_ in zip(ls, us)]
                rs = [v * u_ for v, u_ in zip(rs, us)]

    def interior_z(w, u):
        def body(x, carry):
            for k, d in line_terms(w, u, x, slice(None), 0, CZ):
                acc[k, x] = d
            return carry

        lax.fori_loop(0, nx, body, 0)

    def interior_y(w, u, with_start):
        def body(c, carry):
            rows = pl.ds(pl.multiple_of(c * ROWS, ROWS), ROWS)
            for x in range(nx):
                for k, d in line_terms(w, u, x, rows, 1, CY):
                    acc[k, x, rows, :] += d
                if with_start:
                    power = [w[i, x, rows, :] for i in range(3)]
                    us = [u[i, x, rows, :] for i in range(3)]
                    for k in range(6):
                        start[k, x, rows, :] = total(power)
                        if k < 5:
                            power = [v * u_ for v, u_ in zip(power, us)]
            return carry

        lax.fori_loop(0, chunks, body, 0)

    def edges_yz(s):
        wait_bytes(ry.at[s], sy_r.at[s])
        terms = edge_terms(
            lambda j: packy[s, j], lambda j: ry[s, 0, j], lambda j: ry[s, 1, j], 1, CY
        )
        for k in range(6):
            ey[k] = terms[k]
        wait_bytes(rz.at[s], sz_r.at[s])
        terms = edge_terms(
            lambda j: packz[s, j], lambda j: rz[s, 0, j], lambda j: rz[s, 1, j], 0, CZ
        )
        for k in range(6):
            ez[k] = terms[k]
        for k in range(6):
            for x in range(nx):
                acc[k, x, nz - 2 : nz, :] += ez[k, 4 * x : 4 * x + 2, :]
                acc[k, x, 0:2, :] += ez[k, 4 * x + 2 : 4 * x + 4, :]

    def x_terms(s, c, w, u):
        rows = pl.ds(pl.multiple_of(c * ROWS, ROWS), ROWS)
        lane = lax.broadcasted_iota(jnp.int32, (ROWS, ny), 1)
        edge = (lane < 2) | (lane >= ny - 2)
        ls, rs, us = [], [], []
        for i in range(3):
            wv = [rx[s, c, i, 0], rx[s, c, i, 1]]
            wv += [w[i, x, rows, :] for x in range(nx)]
            wv += [rx[s, c, i, 3], rx[s, c, i, 4]]
            uv = [rx[s, c, i, 2]] + [u[i, x, rows, :] for x in range(nx)] + [rx[s, c, i, 5]]
            jumps = [b - a for a, b in zip(wv[:-1], wv[1:])]
            slopes = [0.5 * minmod(a, b) for a, b in zip(jumps[:-1], jumps[1:])]
            inner = wv[1:-1]
            ls.append([
                (inner[x] + slopes[x]) * (CX * jnp.maximum(uv[x], 0.0)) for x in range(nx + 1)
            ])
            rs.append([
                (inner[x] - slopes[x]) * (CX * jnp.minimum(uv[x], 0.0)) for x in range(1, nx + 2)
            ])
            us.append(uv)
        for k in range(6):
            flux = [
                total([ls[i][x] for i in range(3)]) + total([rs[i][x] for i in range(3)])
                for x in range(nx + 1)
            ]
            for x in range(nx):
                fix = pltpu.roll(ey[k], ny - 2 - 4 * (c * nx + x), 1)
                d = acc[k, x, rows, :] + (flux[x + 1] - flux[x]) + jnp.where(edge, fix, 0.0)
                yield k, x, rows, d
            if k < 5:
                for i in range(3):
                    ls[i] = [v * us[i][x] for x, v in enumerate(ls[i])]
                    rs[i] = [v * us[i][x + 1] for x, v in enumerate(rs[i])]

    def step_of(value):
        return COURANT / (SPEED_TOTAL * jnp.max(value, axis=(0, 1), keepdims=True))

    def tiles_max(value, ref):
        for d in range(ref.shape[0]):
            value = jnp.maximum(value, ref[d])
        return value

    def largest(c, held):
        rows = pl.ds(pl.multiple_of(c * ROWS, ROWS), ROWS)
        for x in range(nx):
            for i in range(3):
                held = jnp.maximum(held, jnp.abs(u1[i, x, rows, :]))
        return held

    zero = jnp.zeros((ROWS, ny), jnp.float32)
    mx[0] = lax.fori_loop(0, chunks, largest, zero)
    loads[0].wait()
    pl.semaphore_wait(barrier, len(peers_a) + len(peers_b))
    send_all(mx.at[0], peers_a, ra.at[0], sa_s.at[0], sa_r.at[0])

    def send_first(c, carry):
        send_x(0, c, w1, u1)
        return carry

    lax.fori_loop(0, chunks, send_first, 0)
    exchange_yz(0, w1, u1)
    interior_z(w1, u1)
    wait_bytes(ra.at[0], sa_r.at[0])
    mx[1] = tiles_max(mx[0], ra.at[0])
    send_all(mx.at[1], peers_b, rb.at[0], sb_s.at[0], sb_r.at[0])
    interior_y(w1, u1, True)
    edges_yz(0)
    wait_bytes(rb.at[0], sb_r.at[0])
    step_one = step_of(tiles_max(mx[1], rb.at[0]))

    def advance(c, held):
        wait_bytes(rx.at[0, c], sx_r.at[0, c])
        rows = pl.ds(pl.multiple_of(c * ROWS, ROWS), ROWS)
        for k, x, rows, d in x_terms(0, c, w1, u1):
            mid[k, x, rows, :] = start[k, x, rows, :] - step_one * d
        for x in range(nx):
            masses, speeds = invert([mid[k, x, rows, :] for k in range(6)])
            for i in range(3):
                w2[i, x, rows, :] = masses[i]
                u2[i, x, rows, :] = speeds[i]
                held = jnp.maximum(held, jnp.abs(speeds[i]))
        send_x(1, c, w2, u2)
        return held

    mx[2] = lax.fori_loop(0, chunks, advance, zero)

    send_all(mx.at[2], peers_b, rb.at[1], sb_s.at[1], sb_r.at[1])
    exchange_yz(1, w2, u2)
    interior_z(w2, u2)
    wait_bytes(rb.at[1], sb_r.at[1])
    mx[3] = tiles_max(mx[2], rb.at[1])
    send_all(mx.at[3], peers_a, ra.at[1], sa_s.at[1], sa_r.at[1])
    interior_y(w2, u2, False)
    edges_yz(1)

    def gather(c, carry):
        wait_bytes(rx.at[1, c], sx_r.at[1, c])
        for k, x, rows, d in x_terms(1, c, w2, u2):
            acc[k, x, rows, :] = d
        return carry

    lax.fori_loop(0, chunks, gather, 0)
    wait_bytes(ra.at[1], sa_r.at[1])
    step_two = step_of(tiles_max(mx[3], ra.at[1]))

    def out_copy(c):
        rows = pl.ds(pl.multiple_of(c * ROWS, ROWS), ROWS)
        return pltpu.make_async_copy(outv.at[:, :, rows], out_hbm.at[:, :, rows], s_out.at[c])

    def finish(c, carry):
        rows = pl.ds(pl.multiple_of(c * ROWS, ROWS), ROWS)
        for k in range(6):
            for x in range(nx):
                at = (k, x, rows, slice(None))
                outv[at] = 0.5 * start[at] + 0.5 * (mid[at] - step_two * acc[at])
        out_copy(c).start()
        return carry

    lax.fori_loop(0, chunks, finish, 0)

    def drain(c, carry):
        out_copy(c).wait()
        for s in range(2):
            wait_bytes(rx.at[s, c], sx_s.at[s, c])
        return carry

    lax.fori_loop(0, chunks, drain, 0)
    for s in range(2):
        wait_bytes(ry.at[s], sy_s.at[s])
        wait_bytes(rz.at[s], sz_s.at[s])
        wait_bytes(ra.at[s], sa_s.at[s])
        wait_bytes(rb.at[s], sb_s.at[s])


def local(sizes, weights, abscissas):
    ngx, ngy, ngz = sizes
    _, nx, nz, ny = weights.shape
    chunks = nz // ROWS
    assert nz % ROWS == 0 and 4 * nx * chunks <= ny and nx >= 2
    assert min(sizes) > 1
    f32 = jnp.float32
    node = pltpu.VMEM((3, nx, nz, ny), f32)
    field = pltpu.VMEM((6, nx, nz, ny), f32)
    dma = pltpu.SemaphoreType.DMA
    na, nb = ngx - 1, ngy * ngz - 1
    any_space = pl.BlockSpec(memory_space=pl.ANY)
    return pl.pallas_call(
        functools.partial(kernel, sizes),
        out_shape=jax.ShapeDtypeStruct((6, nx, nz, ny), f32),
        in_specs=[any_space] * 2,
        out_specs=any_space,
        scratch_shapes=[
            node, node, node, node, field, field, field, field,
            pltpu.VMEM((6, ROWS, ny), f32),
            pltpu.VMEM((6, 4 * nx, ny), f32),
            pltpu.VMEM((2, 6, ROWS, ny), f32),
            pltpu.VMEM((2, 6, 4 * nx, ny), f32),
            pltpu.VMEM((2, chunks, 3, 6, ROWS, ny), f32),
            pltpu.VMEM((2, 2, 6, ROWS, ny), f32),
            pltpu.VMEM((2, 2, 6, 4 * nx, ny), f32),
            pltpu.VMEM((4, ROWS, ny), f32),
            pltpu.VMEM((2, na, ROWS, ny), f32),
            pltpu.VMEM((2, nb, ROWS, ny), f32),
            dma((2,)), dma((chunks,)),
            dma((2, chunks)), dma((2, chunks)),
        ] + [dma((2,))] * 8,
        compiler_params=pltpu.CompilerParams(
            collective_id=0, has_side_effects=True, vmem_limit_bytes=48 * 1024 * 1024
        ),
    )(weights, abscissas)


def solution(mesh):
    sizes = tuple(mesh.shape[a] for a in ("gx", "gy", "gz"))
    spec = P(None, "gx", "gz", "gy")
    return jax.shard_map(
        functools.partial(local, sizes), mesh=mesh, in_specs=(spec, spec), out_specs=spec,
        check_vma=False,
    )
```

```python
import functools

import jax
import jax.numpy as jnp
from jax import lax
from jax.experimental import pallas as pl
from jax.experimental.pallas import tpu as pltpu
from jax.sharding import PartitionSpec as P

MESH = pl.DeviceIdType.MESH
COURANT = 0.4
SPEED_TOTAL = 1.72
CX, CZ, CY = 0.6, 0.64, 0.48
COS_COEFFS = (
    0.500000001, 0.57735016, -0.111107418, 0.0534091939, -0.032581471,
    0.0214679648, -0.0133677689, 0.00671727328, -0.00224476683, 0.000356832615,
)
ROWS = 8


def minmod(a, b):
    return jnp.maximum(jnp.minimum(a, b), 0.0) + jnp.minimum(jnp.maximum(a, b), 0.0)


def third_cos(t):
    acc = jnp.full_like(t, COS_COEFFS[-1])
    for c in COS_COEFFS[-2::-1]:
        acc = acc * t + c
    return acc


def total(parts):
    return parts[0] + parts[1] + parts[2]


def shift(value, amount, axis):
    return pltpu.roll(value, amount % value.shape[axis], axis)


def edge_terms(own, left, right, axis, c):
    shape = own(0).shape
    q = lax.broadcasted_iota(jnp.int32, shape, axis) & 3
    q0, q1, q2 = q == 0, q == 1, q == 2
    dl, dh, dy, us, uxs = [], [], [], [], []
    for i in range(3):
        po, plw, prw = own(i), left(i), right(i)
        u, ux = own(3 + i), jnp.where(q1, left(3 + i), right(3 + i))
        bw, aw = shift(po, 1, axis), shift(po, -1, axis)
        bl, ar = shift(plw, 1, axis), shift(prw, -1, axis)
        bc, ac = jnp.where(q2, bl, bw), jnp.where(q1, ar, aw)
        sc, sw = 0.5 * minmod(po - bc, ac - po), 0.5 * minmod(po - bw, aw - po)
        px = jnp.where(q1, plw, prw)
        bx, ax = jnp.where(q1, bl, bw), jnp.where(q1, aw, ar)
        sx = 0.5 * minmod(px - bx, ax - px)
        up, um = c * jnp.maximum(u, 0.0), c * jnp.minimum(u, 0.0)
        dl.append((sc - sw) * up)
        dh.append((sw - sc) * um)
        wrong = jnp.where(q1, (po + sw) * up, (po - sw) * um)
        outer = jnp.where(
            q1, (px + sx) * (c * jnp.maximum(ux, 0.0)), (px - sx) * (c * jnp.minimum(ux, 0.0))
        )
        dy.append((outer, wrong))
        us.append(u)
        uxs.append(ux)
    result = []
    outer, wrong = [d[0] for d in dy], [d[1] for d in dy]
    for k in range(6):
        a, b = total(dl), total(dh)
        y = total(outer) - total(wrong)
        mid = a - b
        result.append(
            jnp.where(
                q0,
                shift(b, -1, axis),
                jnp.where(
                    q1,
                    mid + shift(y, -1, axis),
                    jnp.where(q2, mid - shift(y, 1, axis), -shift(a, 1, axis)),
                ),
            )
        )
        if k < 5:
            dl = [v * u for v, u in zip(dl, us)]
            dh = [v * u for v, u in zip(dh, us)]
            wrong = [v * u for v, u in zip(wrong, us)]
            outer = [v * u for v, u in zip(outer, uxs)]
    return result


def invert(m):
    inv0 = 1.0 / m[0]
    a0 = m[1] * inv0
    s = [None] + [m[l + 1] - a0 * m[l] for l in range(1, 5)]
    inv1 = 1.0 / s[1]
    lead = s[2] * inv1
    a1 = lead - a0
    b1 = s[1] * inv0
    t2 = s[3] - a1 * s[2] - b1 * m[2]
    t3 = s[4] - a1 * s[3] - b1 * m[3]
    inv2 = 1.0 / t2
    a2 = t3 * inv2 - lead
    b2 = t2 * inv1
    centre = (a0 + a1 + a2) * (1.0 / 3.0)
    d0, d1, d2 = a0 - centre, a1 - centre, a2 - centre
    square = (d0 * d0 + d1 * d1 + d2 * d2 + 2.0 * b1 + 2.0 * b2) * (1.0 / 6.0)
    radius = jnp.sqrt(square)
    det = d0 * d1 * d2 - d0 * b2 - d2 * b1
    half = det / (4.0 * square * radius)
    high = centre + 2.0 * radius * third_cos(jnp.sqrt(jnp.maximum(0.5 + half, 0.0)))
    low = centre - 2.0 * radius * third_cos(jnp.sqrt(jnp.maximum(0.5 - half, 0.0)))
    middle = 3.0 * centre - high - low
    ib1, ib2 = m[0] * inv1, s[1] * inv2
    masses = []
    for value in (low, middle, high):
        d = value - a0
        e = (value - a1) * d - b1
        masses.append(m[0] / (1.0 + ib1 * (d * d + ib2 * (e * e))))
    return masses, (low, middle, high)


def kernel(
    sizes, w_hbm, u_hbm, out_hbm, w1, u1, w2, u2, start, mid, acc, out, ey, ez,
    packy, packz, rx, ry, rz, mx, ra, rb,
    s_in, s_out, sx_s, sx_r, sy_s, sy_r, sz_s, sz_r, sa_s, sa_r, sb_s, sb_r,
):
    ngx, ngy, ngz = sizes
    gx, gy, gz = (lax.axis_index(a) for a in ("gx", "gy", "gz"))
    _, nx, nz, ny = w1.shape
    chunks = nz // ROWS
    xdown, xup = {"gx": lax.rem(gx + ngx - 1, ngx)}, {"gx": lax.rem(gx + 1, ngx)}
    ydown, yup = {"gy": lax.rem(gy + ngy - 1, ngy)}, {"gy": lax.rem(gy + 1, ngy)}
    zdown, zup = {"gz": lax.rem(gz + ngz - 1, ngz)}, {"gz": lax.rem(gz + 1, ngz)}
    peers_a = [{"gx": lax.rem(gx + d, ngx)} for d in range(1, ngx)]
    flat = gy * ngz + gz
    peers_b = []
    for d in range(1, ngy * ngz):
        other = lax.rem(flat + d, ngy * ngz)
        peers_b.append({"gy": lax.div(other, ngz), "gz": lax.rem(other, ngz)})

    loads = [
        pltpu.make_async_copy(w_hbm, w1, s_in.at[0]),
        pltpu.make_async_copy(u_hbm, u1, s_in.at[1]),
    ]
    for copy in loads:
        copy.start()
    barrier = pltpu.get_barrier_semaphore()
    for peer in peers_a + peers_b:
        pl.semaphore_signal(barrier, inc=1, device_id=peer, device_id_type=MESH)
    loads[1].wait()

    def remote(src, dst, send, recv, peer):
        pltpu.make_async_remote_copy(
            src_ref=src, dst_ref=dst, send_sem=send, recv_sem=recv,
            device_id=peer, device_id_type=MESH,
        ).start()

    def wait_bytes(ref, sem):
        pltpu.make_async_copy(ref, ref, sem).wait()

    def send_all(src, peers, dst, send, recv):
        for d, peer in enumerate(peers):
            remote(src, dst.at[d], send, recv, peer)

    def send_x(s, c, w, u):
        rows = pl.ds(pl.multiple_of(c * ROWS, ROWS), ROWS)
        dst, send, recv = rx.at[s, c], sx_s.at[s, c], sx_r.at[s, c]
        remote(w.at[:, 0:2, rows], dst.at[:, 3:5], send, recv, xdown)
        remote(w.at[:, nx - 2 : nx, rows], dst.at[:, 0:2], send, recv, xup)
        remote(u.at[:, 0:1, rows], dst.at[:, 5:6], send, recv, xdown)
        remote(u.at[:, nx - 1 : nx, rows], dst.at[:, 2:3], send, recv, xup)

    def exchange_yz(s, w, u):
        lane = lax.broadcasted_iota(jnp.int32, (ROWS, ny), 1) >> 2

        def pack(c, held):
            rows = pl.ds(pl.multiple_of(c * ROWS, ROWS), ROWS)
            held = list(held)
            for x in range(nx):
                p = c * nx + x
                for i in range(3):
                    for j, ref in ((i, w), (3 + i, u)):
                        moved = pltpu.roll(ref[i, x, rows, :], 4 * p + 2, 1)
                        held[j] = jnp.where(lane == p, moved, held[j])
            return tuple(held)

        held = lax.fori_loop(
            0, chunks, pack, tuple(jnp.zeros((ROWS, ny), jnp.float32) for _ in range(6))
        )
        for j in range(6):
            packy[s, j] = held[j]
        for i in range(3):
            for x in range(nx):
                for j, ref in ((i, w), (3 + i, u)):
                    packz[s, j, 4 * x : 4 * x + 2, :] = ref[i, x, nz - 2 : nz, :]
                    packz[s, j, 4 * x + 2 : 4 * x + 4, :] = ref[i, x, 0:2, :]
        remote(packy.at[s], ry.at[s, 1], sy_s.at[s], sy_r.at[s], ydown)
        remote(packy.at[s], ry.at[s, 0], sy_s.at[s], sy_r.at[s], yup)
        remote(packz.at[s], rz.at[s, 1], sz_s.at[s], sz_r.at[s], zdown)
        remote(packz.at[s], rz.at[s, 0], sz_s.at[s], sz_r.at[s], zup)

    def line_terms(w, u, x, rows, axis, c):
        ls, rs, us = [], [], []
        for i in range(3):
            wv, uv = w[i, x, rows, :], u[i, x, rows, :]
            jump = wv - shift(wv, 1, axis)
            s = 0.5 * minmod(jump, shift(jump, -1, axis))
            ls.append((wv + s) * (c * jnp.maximum(uv, 0.0)))
            rs.append((wv - s) * (c * jnp.minimum(uv, 0.0)))
            us.append(uv)
        for k in range(6):
            g, h = total(ls), total(rs)
            yield k, (g - h) - shift(g, 1, axis) + shift(h, -1, axis)
            if k < 5:
                ls = [v * u_ for v, u_ in zip(ls, us)]
                rs = [v * u_ for v, u_ in zip(rs, us)]

    def interior_z(w, u):
        def body(x, carry):
            for k, d in line_terms(w, u, x, slice(None), 0, CZ):
                acc[k, x] = d
            return carry

        lax.fori_loop(0, nx, body, 0)

    def interior_y(w, u, with_start):
        def body(c, carry):
            rows = pl.ds(pl.multiple_of(c * ROWS, ROWS), ROWS)
            for x in range(nx):
                for k, d in line_terms(w, u, x, rows, 1, CY):
                    acc[k, x, rows, :] += d
                if with_start:
                    power = [w[i, x, rows, :] for i in range(3)]
                    us = [u[i, x, rows, :] for i in range(3)]
                    for k in range(6):
                        start[k, x, rows, :] = total(power)
                        if k < 5:
                            power = [v * u_ for v, u_ in zip(power, us)]
            return carry

        lax.fori_loop(0, chunks, body, 0)

    def edges_yz(s):
        wait_bytes(ry.at[s], sy_r.at[s])
        terms = edge_terms(
            lambda j: packy[s, j], lambda j: ry[s, 0, j], lambda j: ry[s, 1, j], 1, CY
        )
        for k in range(6):
            ey[k] = terms[k]
        wait_bytes(rz.at[s], sz_r.at[s])
        terms = edge_terms(
            lambda j: packz[s, j], lambda j: rz[s, 0, j], lambda j: rz[s, 1, j], 0, CZ
        )
        for k in range(6):
            ez[k] = terms[k]
        for k in range(6):
            for x in range(nx):
                acc[k, x, nz - 2 : nz, :] += ez[k, 4 * x : 4 * x + 2, :]
                acc[k, x, 0:2, :] += ez[k, 4 * x + 2 : 4 * x + 4, :]

    def x_terms(s, c, w, u):
        rows = pl.ds(pl.multiple_of(c * ROWS, ROWS), ROWS)
        lane = lax.broadcasted_iota(jnp.int32, (ROWS, ny), 1)
        edge = (lane < 2) | (lane >= ny - 2)
        ls, rs, us = [], [], []
        for i in range(3):
            wv = [rx[s, c, i, 0], rx[s, c, i, 1]]
            wv += [w[i, x, rows, :] for x in range(nx)]
            wv += [rx[s, c, i, 3], rx[s, c, i, 4]]
            uv = [rx[s, c, i, 2]] + [u[i, x, rows, :] for x in range(nx)] + [rx[s, c, i, 5]]
            jumps = [b - a for a, b in zip(wv[:-1], wv[1:])]
            slopes = [0.5 * minmod(a, b) for a, b in zip(jumps[:-1], jumps[1:])]
            inner = wv[1:-1]
            ls.append([
                (inner[x] + slopes[x]) * (CX * jnp.maximum(uv[x], 0.0)) for x in range(nx + 1)
            ])
            rs.append([
                (inner[x] - slopes[x]) * (CX * jnp.minimum(uv[x], 0.0)) for x in range(1, nx + 2)
            ])
            us.append(uv)
        for k in range(6):
            flux = [
                total([ls[i][x] for i in range(3)]) + total([rs[i][x] for i in range(3)])
                for x in range(nx + 1)
            ]
            for x in range(nx):
                fix = pltpu.roll(ey[k], ny - 2 - 4 * (c * nx + x), 1)
                d = acc[k, x, rows, :] + (flux[x + 1] - flux[x]) + jnp.where(edge, fix, 0.0)
                yield k, x, rows, d
            if k < 5:
                for i in range(3):
                    ls[i] = [v * us[i][x] for x, v in enumerate(ls[i])]
                    rs[i] = [v * us[i][x + 1] for x, v in enumerate(rs[i])]

    def step_of(value):
        return COURANT / (SPEED_TOTAL * jnp.max(value, axis=(0, 1), keepdims=True))

    def tiles_max(value, ref):
        for d in range(ref.shape[0]):
            value = jnp.maximum(value, ref[d])
        return value

    def largest(c, held):
        rows = pl.ds(pl.multiple_of(c * ROWS, ROWS), ROWS)
        for x in range(nx):
            for i in range(3):
                held = jnp.maximum(held, jnp.abs(u1[i, x, rows, :]))
        return held

    zero = jnp.zeros((ROWS, ny), jnp.float32)
    mx[0] = lax.fori_loop(0, chunks, largest, zero)
    loads[0].wait()
    pl.semaphore_wait(barrier, len(peers_a) + len(peers_b))
    send_all(mx.at[0], peers_a, ra.at[0], sa_s.at[0], sa_r.at[0])

    def send_first(c, carry):
        send_x(0, c, w1, u1)
        return carry

    lax.fori_loop(0, chunks, send_first, 0)
    exchange_yz(0, w1, u1)
    interior_z(w1, u1)
    wait_bytes(ra.at[0], sa_r.at[0])
    mx[1] = tiles_max(mx[0], ra.at[0])
    send_all(mx.at[1], peers_b, rb.at[0], sb_s.at[0], sb_r.at[0])
    interior_y(w1, u1, True)
    edges_yz(0)
    wait_bytes(rb.at[0], sb_r.at[0])
    step_one = step_of(tiles_max(mx[1], rb.at[0]))

    early = chunks - 2

    def advance(c, held):
        wait_bytes(rx.at[0, c], sx_r.at[0, c])
        rows = pl.ds(pl.multiple_of(c * ROWS, ROWS), ROWS)
        for k, x, rows, d in x_terms(0, c, w1, u1):
            mid[k, x, rows, :] = start[k, x, rows, :] - step_one * d
        for x in range(nx):
            masses, speeds = invert([mid[k, x, rows, :] for k in range(6)])
            for i in range(3):
                w2[i, x, rows, :] = masses[i]
                u2[i, x, rows, :] = speeds[i]
                held = jnp.maximum(held, jnp.abs(speeds[i]))
        @pl.when(c < early)
        def _():
            send_x(1, c, w2, u2)

        return held

    mx[2] = lax.fori_loop(0, chunks, advance, zero)

    send_all(mx.at[2], peers_b, rb.at[1], sb_s.at[1], sb_r.at[1])
    exchange_yz(1, w2, u2)
    interior_z(w2, u2)
    wait_bytes(rb.at[1], sb_r.at[1])
    mx[3] = tiles_max(mx[2], rb.at[1])
    send_all(mx.at[3], peers_a, ra.at[1], sa_s.at[1], sa_r.at[1])
    def send_late(c, carry):
        send_x(1, c, w2, u2)
        return carry

    lax.fori_loop(early, chunks, send_late, 0)
    interior_y(w2, u2, False)
    edges_yz(1)
    wait_bytes(ra.at[1], sa_r.at[1])
    step_two = step_of(tiles_max(mx[3], ra.at[1]))

    def out_copy(c):
        rows = pl.ds(pl.multiple_of(c * ROWS, ROWS), ROWS)
        return pltpu.make_async_copy(out.at[:, :, rows], out_hbm.at[:, :, rows], s_out.at[c])

    def finish(c, carry):
        wait_bytes(rx.at[1, c], sx_r.at[1, c])
        for k, x, rows, d in x_terms(1, c, w2, u2):
            at = (k, x, rows, slice(None))
            out[at] = 0.5 * start[at] + 0.5 * (mid[at] - step_two * d)
        out_copy(c).start()
        return carry

    lax.fori_loop(0, chunks, finish, 0)

    def drain(c, carry):
        out_copy(c).wait()
        for s in range(2):
            wait_bytes(rx.at[s, c], sx_s.at[s, c])
        return carry

    lax.fori_loop(0, chunks, drain, 0)
    for s in range(2):
        wait_bytes(ry.at[s], sy_s.at[s])
        wait_bytes(rz.at[s], sz_s.at[s])
        wait_bytes(ra.at[s], sa_s.at[s])
        wait_bytes(rb.at[s], sb_s.at[s])


def local(sizes, weights, abscissas):
    ngx, ngy, ngz = sizes
    _, nx, nz, ny = weights.shape
    chunks = nz // ROWS
    assert nz % ROWS == 0 and 4 * nx * chunks <= ny and nx >= 2
    assert min(sizes) > 1
    f32 = jnp.float32
    node = pltpu.VMEM((3, nx, nz, ny), f32)
    field = pltpu.VMEM((6, nx, nz, ny), f32)
    dma = pltpu.SemaphoreType.DMA
    na, nb = ngx - 1, ngy * ngz - 1
    return pl.pallas_call(
        functools.partial(kernel, sizes),
        out_shape=jax.ShapeDtypeStruct((6, nx, nz, ny), f32),
        in_specs=[pl.BlockSpec(memory_space=pltpu.HBM)] * 2,
        out_specs=pl.BlockSpec(memory_space=pltpu.HBM),
        scratch_shapes=[
            node, node, node, node, field, field, field, field,
            pltpu.VMEM((6, ROWS, ny), f32),
            pltpu.VMEM((6, 4 * nx, ny), f32),
            pltpu.VMEM((2, 6, ROWS, ny), f32),
            pltpu.VMEM((2, 6, 4 * nx, ny), f32),
            pltpu.VMEM((2, chunks, 3, 6, ROWS, ny), f32),
            pltpu.VMEM((2, 2, 6, ROWS, ny), f32),
            pltpu.VMEM((2, 2, 6, 4 * nx, ny), f32),
            pltpu.VMEM((4, ROWS, ny), f32),
            pltpu.VMEM((2, na, ROWS, ny), f32),
            pltpu.VMEM((2, nb, ROWS, ny), f32),
            dma((2,)), dma((chunks,)),
            dma((2, chunks)), dma((2, chunks)),
        ] + [dma((2,))] * 8,
        compiler_params=pltpu.CompilerParams(
            collective_id=0, has_side_effects=True, vmem_limit_bytes=67043328
        ),
    )(weights, abscissas)


def solution(mesh):
    sizes = tuple(mesh.shape[a] for a in ("gx", "gy", "gz"))
    spec = P(None, "gx", "gz", "gy")
    return jax.shard_map(
        functools.partial(local, sizes), mesh=mesh, in_specs=(spec, spec), out_specs=spec,
        check_vma=False,
    )
```

```python
import functools

import jax
import jax.numpy as jnp
from jax import lax
from jax.experimental import pallas as pl
from jax.experimental.pallas import tpu as pltpu
from jax.sharding import PartitionSpec as P

MESH = pl.DeviceIdType.MESH
COURANT = 0.4
SPEED_TOTAL = 1.72
CX, CZ, CY = 0.6, 0.64, 0.48
COS_COEFFS = (
    0.500000001, 0.57735016, -0.111107418, 0.0534091939, -0.032581471,
    0.0214679648, -0.0133677689, 0.00671727328, -0.00224476683, 0.000356832615,
)
ROWS = 8


def minmod(a, b):
    return jnp.maximum(jnp.minimum(a, b), 0.0) + jnp.minimum(jnp.maximum(a, b), 0.0)


def third_cos(t):
    acc = jnp.full_like(t, COS_COEFFS[-1])
    for c in COS_COEFFS[-2::-1]:
        acc = acc * t + c
    return acc


def total(parts):
    return parts[0] + parts[1] + parts[2]


def shift(value, amount, axis):
    return pltpu.roll(value, amount % value.shape[axis], axis)


def edge_terms(own, left, right, axis, c):
    shape = own(0).shape
    q = lax.broadcasted_iota(jnp.int32, shape, axis) & 3
    q0, q1, q2 = q == 0, q == 1, q == 2
    dl, dh, dy, us, uxs = [], [], [], [], []
    for i in range(3):
        po, plw, prw = own(i), left(i), right(i)
        u, ux = own(3 + i), jnp.where(q1, left(3 + i), right(3 + i))
        bw, aw = shift(po, 1, axis), shift(po, -1, axis)
        bl, ar = shift(plw, 1, axis), shift(prw, -1, axis)
        bc, ac = jnp.where(q2, bl, bw), jnp.where(q1, ar, aw)
        sc, sw = 0.5 * minmod(po - bc, ac - po), 0.5 * minmod(po - bw, aw - po)
        px = jnp.where(q1, plw, prw)
        bx, ax = jnp.where(q1, bl, bw), jnp.where(q1, aw, ar)
        sx = 0.5 * minmod(px - bx, ax - px)
        up, um = c * jnp.maximum(u, 0.0), c * jnp.minimum(u, 0.0)
        dl.append((sc - sw) * up)
        dh.append((sw - sc) * um)
        wrong = jnp.where(q1, (po + sw) * up, (po - sw) * um)
        outer = jnp.where(
            q1, (px + sx) * (c * jnp.maximum(ux, 0.0)), (px - sx) * (c * jnp.minimum(ux, 0.0))
        )
        dy.append((outer, wrong))
        us.append(u)
        uxs.append(ux)
    result = []
    outer, wrong = [d[0] for d in dy], [d[1] for d in dy]
    for k in range(6):
        a, b = total(dl), total(dh)
        y = total(outer) - total(wrong)
        mid = a - b
        result.append(
            jnp.where(
                q0,
                shift(b, -1, axis),
                jnp.where(
                    q1,
                    mid + shift(y, -1, axis),
                    jnp.where(q2, mid - shift(y, 1, axis), -shift(a, 1, axis)),
                ),
            )
        )
        if k < 5:
            dl = [v * u for v, u in zip(dl, us)]
            dh = [v * u for v, u in zip(dh, us)]
            wrong = [v * u for v, u in zip(wrong, us)]
            outer = [v * u for v, u in zip(outer, uxs)]
    return result


def invert(m):
    inv0 = 1.0 / m[0]
    a0 = m[1] * inv0
    s = [None] + [m[l + 1] - a0 * m[l] for l in range(1, 5)]
    inv1 = 1.0 / s[1]
    lead = s[2] * inv1
    a1 = lead - a0
    b1 = s[1] * inv0
    t2 = s[3] - a1 * s[2] - b1 * m[2]
    t3 = s[4] - a1 * s[3] - b1 * m[3]
    inv2 = 1.0 / t2
    a2 = t3 * inv2 - lead
    b2 = t2 * inv1
    centre = (a0 + a1 + a2) * (1.0 / 3.0)
    d0, d1, d2 = a0 - centre, a1 - centre, a2 - centre
    square = (d0 * d0 + d1 * d1 + d2 * d2 + 2.0 * b1 + 2.0 * b2) * (1.0 / 6.0)
    radius = jnp.sqrt(square)
    det = d0 * d1 * d2 - d0 * b2 - d2 * b1
    half = det / (4.0 * square * radius)
    high = centre + 2.0 * radius * third_cos(jnp.sqrt(jnp.maximum(0.5 + half, 0.0)))
    low = centre - 2.0 * radius * third_cos(jnp.sqrt(jnp.maximum(0.5 - half, 0.0)))
    middle = 3.0 * centre - high - low
    ib1, ib2 = m[0] * inv1, s[1] * inv2
    masses = []
    for value in (low, middle, high):
        d = value - a0
        e = (value - a1) * d - b1
        masses.append(m[0] / (1.0 + ib1 * (d * d + ib2 * (e * e))))
    return masses, (low, middle, high)


def kernel(
    sizes, w_hbm, u_hbm, out, n1, n2, start, mid, acc, ey, ez,
    packy, packz, rx, ry, rz, mx, ra, rb,
    s_in, sx_s, sx_r, sy_s, sy_r, sz_s, sz_r, sa_s, sa_r, sb_s, sb_r,
):
    ngx, ngy, ngz = sizes
    gx, gy, gz = (lax.axis_index(a) for a in ("gx", "gy", "gz"))
    chunks, planes, _, ny = n1.shape
    nx, nz = planes // 6, chunks * ROWS
    xdown, xup = {"gx": lax.rem(gx + ngx - 1, ngx)}, {"gx": lax.rem(gx + 1, ngx)}
    ydown, yup = {"gy": lax.rem(gy + ngy - 1, ngy)}, {"gy": lax.rem(gy + 1, ngy)}
    zdown, zup = {"gz": lax.rem(gz + ngz - 1, ngz)}, {"gz": lax.rem(gz + 1, ngz)}
    peers_a = [{"gx": lax.rem(gx + d, ngx)} for d in range(1, ngx)]
    flat = gy * ngz + gz
    peers_b = []
    for d in range(1, ngy * ngz):
        other = lax.rem(flat + d, ngy * ngz)
        peers_b.append({"gy": lax.div(other, ngz), "gz": lax.rem(other, ngz)})

    def first(x):
        late = 3 * (x >= nx // 2) if isinstance(x, int) else jnp.where(x >= nx // 2, 3, 0)
        return 6 * x + late, 6 * x + 3 - late

    def w_at(x, i):
        return first(x)[0] + i

    def u_at(x, i):
        return first(x)[1] + i

    for x in range(nx):
        for i in range(3):
            pltpu.make_async_copy(u_hbm.at[i, x], n1.at[:, u_at(x, i)], s_in.at[0]).start()
            pltpu.make_async_copy(w_hbm.at[i, x], n1.at[:, w_at(x, i)], s_in.at[0]).start()
    barrier = pltpu.get_barrier_semaphore()
    for peer in peers_a + peers_b:
        pl.semaphore_signal(barrier, inc=1, device_id=peer, device_id_type=MESH)

    def remote(src, dst, send, recv, peer):
        pltpu.make_async_remote_copy(
            src_ref=src, dst_ref=dst, send_sem=send, recv_sem=recv,
            device_id=peer, device_id_type=MESH,
        ).start()

    def wait_bytes(ref, sem):
        pltpu.make_async_copy(ref, ref, sem).wait()

    def send_all(src, peers, dst, send, recv):
        for d, peer in enumerate(peers):
            remote(src, dst.at[d], send, recv, peer)

    def send_x(s, c, n):
        send, recv = sx_s.at[s, c], sx_r.at[s, c]
        @pl.when(gx == 0)
        def _():
            remote(n.at[c, 0:9], rx.at[s, c, 9:18], send, recv, xdown)

        remote(n.at[c, planes - 9 : planes], rx.at[s, c, 0:9], send, recv, xup)

        @pl.when(gx != 0)
        def _():
            remote(n.at[c, 0:9], rx.at[s, c, 9:18], send, recv, xdown)


    def exchange_yz(s, n):
        lane = lax.broadcasted_iota(jnp.int32, (ROWS, ny), 1) >> 2

        def pack(c, held):
            held = list(held)
            for x in range(nx):
                p = c * nx + x
                for i in range(3):
                    for j, at in ((i, w_at(x, i)), (3 + i, u_at(x, i))):
                        moved = pltpu.roll(n[c, at], 4 * p + 2, 1)
                        held[j] = jnp.where(lane == p, moved, held[j])
            return tuple(held)

        held = lax.fori_loop(
            0, chunks, pack, tuple(jnp.zeros((ROWS, ny), jnp.float32) for _ in range(6))
        )
        for j in range(6):
            packy[s, j] = held[j]
        for i in range(3):
            for x in range(nx):
                for j, at in ((i, w_at(x, i)), (3 + i, u_at(x, i))):
                    packz[s, j, 4 * x : 4 * x + 2, :] = n[chunks - 1, at, ROWS - 2 : ROWS, :]
                    packz[s, j, 4 * x + 2 : 4 * x + 4, :] = n[0, at, 0:2, :]
        remote(packy.at[s], ry.at[s, 1], sy_s.at[s], sy_r.at[s], ydown)
        remote(packy.at[s], ry.at[s, 0], sy_s.at[s], sy_r.at[s], yup)
        remote(packz.at[s], rz.at[s, 1], sz_s.at[s], sz_r.at[s], zdown)
        remote(packz.at[s], rz.at[s, 0], sz_s.at[s], sz_r.at[s], zup)

    def line_terms(load, axis, c):
        ls, rs, us = [], [], []
        for i in range(3):
            wv, uv = load(i)
            jump = wv - shift(wv, 1, axis)
            s = 0.5 * minmod(jump, shift(jump, -1, axis))
            ls.append((wv + s) * (c * jnp.maximum(uv, 0.0)))
            rs.append((wv - s) * (c * jnp.minimum(uv, 0.0)))
            us.append(uv)
        for k in range(6):
            g, h = total(ls), total(rs)
            yield k, (g - h) - shift(g, 1, axis) + shift(h, -1, axis)
            if k < 5:
                ls = [v * u_ for v, u_ in zip(ls, us)]
                rs = [v * u_ for v, u_ in zip(rs, us)]

    def interior_z(n):
        def body(x, carry):
            def load(i):
                column = (nz, ny)
                return n[:, w_at(x, i)].reshape(column), n[:, u_at(x, i)].reshape(column)

            for k, d in line_terms(load, 0, CZ):
                acc[k, x] = d
            return carry

        lax.fori_loop(0, nx, body, 0)

    def interior_y(n, with_start):
        def body(c, carry):
            rows = pl.ds(pl.multiple_of(c * ROWS, ROWS), ROWS)
            for x in range(nx):
                def load(i, x=x):
                    return n[c, w_at(x, i)], n[c, u_at(x, i)]

                for k, d in line_terms(load, 1, CY):
                    acc[k, x, rows, :] += d
                if with_start:
                    power = [n[c, w_at(x, i)] for i in range(3)]
                    us = [n[c, u_at(x, i)] for i in range(3)]
                    for k in range(6):
                        start[k, x, rows, :] = total(power)
                        if k < 5:
                            power = [v * u_ for v, u_ in zip(power, us)]
            return carry

        lax.fori_loop(0, chunks, body, 0)

    def edges_yz(s):
        wait_bytes(ry.at[s], sy_r.at[s])
        terms = edge_terms(
            lambda j: packy[s, j], lambda j: ry[s, 0, j], lambda j: ry[s, 1, j], 1, CY
        )
        for k in range(6):
            ey[k] = terms[k]
        wait_bytes(rz.at[s], sz_r.at[s])
        terms = edge_terms(
            lambda j: packz[s, j], lambda j: rz[s, 0, j], lambda j: rz[s, 1, j], 0, CZ
        )
        for k in range(6):
            ez[k] = terms[k]
        for k in range(6):
            for x in range(nx):
                acc[k, x, nz - 2 : nz, :] += ez[k, 4 * x : 4 * x + 2, :]
                acc[k, x, 0:2, :] += ez[k, 4 * x + 2 : 4 * x + 4, :]

    def x_terms(s, c, n):
        rows = pl.ds(pl.multiple_of(c * ROWS, ROWS), ROWS)
        lane = lax.broadcasted_iota(jnp.int32, (ROWS, ny), 1)
        edge = (lane < 2) | (lane >= ny - 2)
        ls, rs, us = [], [], []
        for i in range(3):
            wv = [rx[s, c, i], rx[s, c, 6 + i]]
            wv += [n[c, w_at(x, i)] for x in range(nx)]
            wv += [rx[s, c, 9 + i], rx[s, c, 15 + i]]
            uv = [rx[s, c, 3 + i]] + [n[c, u_at(x, i)] for x in range(nx)] + [rx[s, c, 12 + i]]
            jumps = [b - a for a, b in zip(wv[:-1], wv[1:])]
            slopes = [0.5 * minmod(a, b) for a, b in zip(jumps[:-1], jumps[1:])]
            inner = wv[1:-1]
            ls.append([
                (inner[x] + slopes[x]) * (CX * jnp.maximum(uv[x], 0.0)) for x in range(nx + 1)
            ])
            rs.append([
                (inner[x] - slopes[x]) * (CX * jnp.minimum(uv[x], 0.0)) for x in range(1, nx + 2)
            ])
            us.append(uv)
        for k in range(6):
            flux = [
                total([ls[i][x] for i in range(3)]) + total([rs[i][x] for i in range(3)])
                for x in range(nx + 1)
            ]
            for x in range(nx):
                fix = pltpu.roll(ey[k], ny - 2 - 4 * (c * nx + x), 1)
                d = acc[k, x, rows, :] + (flux[x + 1] - flux[x]) + jnp.where(edge, fix, 0.0)
                yield k, x, rows, d
            if k < 5:
                for i in range(3):
                    ls[i] = [v * us[i][x] for x, v in enumerate(ls[i])]
                    rs[i] = [v * us[i][x + 1] for x, v in enumerate(rs[i])]

    def step_of(value):
        return COURANT / (SPEED_TOTAL * jnp.max(value, axis=(0, 1), keepdims=True))

    def tiles_max(value, ref):
        for d in range(ref.shape[0]):
            value = jnp.maximum(value, ref[d])
        return value

    def largest(c, held):
        for x in range(nx):
            for i in range(3):
                held = jnp.maximum(held, jnp.abs(n1[c, u_at(x, i)]))
        return held

    zero = jnp.zeros((ROWS, ny), jnp.float32)
    wait_bytes(n1, s_in.at[0])
    mx[0] = lax.fori_loop(0, chunks, largest, zero)
    pl.semaphore_wait(barrier, len(peers_a) + len(peers_b))
    send_all(mx.at[0], peers_a, ra.at[0], sa_s.at[0], sa_r.at[0])

    def send_first(c, carry):
        send_x(0, c, n1)
        return carry

    lax.fori_loop(0, chunks, send_first, 0)
    exchange_yz(0, n1)
    interior_z(n1)
    wait_bytes(ra.at[0], sa_r.at[0])
    mx[1] = tiles_max(mx[0], ra.at[0])
    send_all(mx.at[1], peers_b, rb.at[0], sb_s.at[0], sb_r.at[0])
    interior_y(n1, True)
    edges_yz(0)
    wait_bytes(rb.at[0], sb_r.at[0])
    step_one = step_of(tiles_max(mx[1], rb.at[0]))

    early = chunks - 2

    def advance(c, held):
        wait_bytes(rx.at[0, c], sx_r.at[0, c])
        rows = pl.ds(pl.multiple_of(c * ROWS, ROWS), ROWS)
        for k, x, rows, d in x_terms(0, c, n1):
            mid[k, x, rows, :] = start[k, x, rows, :] - step_one * d
        for x in range(nx):
            masses, speeds = invert([mid[k, x, rows, :] for k in range(6)])
            for i in range(3):
                n2[c, w_at(x, i)] = masses[i]
                n2[c, u_at(x, i)] = speeds[i]
                held = jnp.maximum(held, jnp.abs(speeds[i]))
        @pl.when(c < early)
        def _():
            send_x(1, c, n2)

        return held

    mx[2] = lax.fori_loop(0, chunks, advance, zero)

    send_all(mx.at[2], peers_b, rb.at[1], sb_s.at[1], sb_r.at[1])
    exchange_yz(1, n2)
    interior_z(n2)
    wait_bytes(rb.at[1], sb_r.at[1])
    mx[3] = tiles_max(mx[2], rb.at[1])
    send_all(mx.at[3], peers_a, ra.at[1], sa_s.at[1], sa_r.at[1])
    def send_late(c, carry):
        send_x(1, c, n2)
        return carry

    lax.fori_loop(early, chunks, send_late, 0)
    interior_y(n2, False)
    edges_yz(1)
    wait_bytes(ra.at[1], sa_r.at[1])
    step_two = step_of(tiles_max(mx[3], ra.at[1]))

    def finish(c, carry):
        wait_bytes(rx.at[1, c], sx_r.at[1, c])
        for k, x, rows, d in x_terms(1, c, n2):
            at = (k, x, rows, slice(None))
            out[at] = 0.5 * start[at] + 0.5 * (mid[at] - step_two * d)
        return carry

    lax.fori_loop(0, chunks, finish, 0)

    def drain(c, carry):
        for s in range(2):
            wait_bytes(rx.at[s, c], sx_s.at[s, c])
        return carry

    lax.fori_loop(0, chunks, drain, 0)
    for s in range(2):
        wait_bytes(ry.at[s], sy_s.at[s])
        wait_bytes(rz.at[s], sz_s.at[s])
        wait_bytes(ra.at[s], sa_s.at[s])
        wait_bytes(rb.at[s], sb_s.at[s])


def local(sizes, weights, abscissas):
    ngx, ngy, ngz = sizes
    _, nx, nz, ny = weights.shape
    chunks = nz // ROWS
    assert nz % ROWS == 0 and 4 * nx * chunks <= ny and nx >= 4
    assert min(sizes) > 1
    f32 = jnp.float32
    node = pltpu.VMEM((chunks, 6 * nx, ROWS, ny), f32)
    field = pltpu.VMEM((6, nx, nz, ny), f32)
    dma = pltpu.SemaphoreType.DMA
    na, nb = ngx - 1, ngy * ngz - 1
    return pl.pallas_call(
        functools.partial(kernel, sizes),
        out_shape=pltpu.VMEM((6, nx, nz, ny), f32),
        in_specs=[pl.BlockSpec(memory_space=pltpu.HBM)] * 2,
        out_specs=pl.BlockSpec(memory_space=pltpu.VMEM),
        scratch_shapes=[
            node, node, field, field, field,
            pltpu.VMEM((6, ROWS, ny), f32),
            pltpu.VMEM((6, 4 * nx, ny), f32),
            pltpu.VMEM((2, 6, ROWS, ny), f32),
            pltpu.VMEM((2, 6, 4 * nx, ny), f32),
            pltpu.VMEM((2, chunks, 18, ROWS, ny), f32),
            pltpu.VMEM((2, 2, 6, ROWS, ny), f32),
            pltpu.VMEM((2, 2, 6, 4 * nx, ny), f32),
            pltpu.VMEM((4, ROWS, ny), f32),
            pltpu.VMEM((2, na, ROWS, ny), f32),
            pltpu.VMEM((2, nb, ROWS, ny), f32),
            dma((2,)),
            dma((2, chunks)), dma((2, chunks)),
        ] + [dma((2,))] * 8,
        compiler_params=pltpu.CompilerParams(
            collective_id=0, has_side_effects=True, vmem_limit_bytes=56000000
        ),
    )(*(a.reshape(3, nx, chunks, ROWS, ny) for a in (weights, abscissas)))


def solution(mesh):
    sizes = tuple(mesh.shape[a] for a in ("gx", "gy", "gz"))
    spec = P(None, "gx", "gz", "gy")
    return jax.shard_map(
        functools.partial(local, sizes), mesh=mesh, in_specs=(spec, spec), out_specs=spec,
        check_vma=False,
    )
```
